32 devices in a mesh: dp: 2 (over z, core), tp: 16 (over x, y).
Axes of the slice: x: 4, y: 4, z: 1, core: 2. Of those that a mesh axis runs over, the one named last changes fastest.
The devices are a block of a 4x4x8 slice.
Arguments:
- x: bfloat16 [8192, 4096], P(('dp', 'tp')), parts along dimension 0
- w_gate: bfloat16 [4096, 16384], P(None, 'tp')
- w_up: bfloat16 [4096, 16384], P(None, 'tp')
- w_down: bfloat16 [16384, 4096], P('tp')
Outputs:
- output: bfloat16 [8192, 4096], P(('dp', 'tp')), parts along dimension 0
There are 2 independent parts. The reference program is written for one: setup_inputs(seed, part) draws one part's arguments, and reference() takes and returns one part's arrays. A program takes and returns all parts, laid end to end along the dimension named above; an argument that names none is the same for every part.
All inputs are finite; a program needn't handle non-finite values.
Results may differ from the reference program's by a relative error of at most 0.016.
Values are sent between devices in bfloat16 or wider.
A program may use at most 768 MiB of HBM per device.

```python
import jax
import jax.numpy as jnp

ROWS = 4096
D = 4096
FF = 16384


def setup_inputs(seed: int = 0, part: int = 0) -> dict:
    kx, kg, ku, kd = jax.random.split(jax.random.key(seed), 4)
    drawn = {
        "x": jax.random.normal(jax.random.fold_in(kx, part), (ROWS, D), jnp.float32),
        "w_gate": jax.random.normal(kg, (D, FF), jnp.float32) * D**-0.5,
        "w_up": jax.random.normal(ku, (D, FF), jnp.float32) * D**-0.5,
        "w_down": jax.random.normal(kd, (FF, D), jnp.float32) * FF**-0.5,
    }
    return {k: v.astype(jnp.bfloat16) for k, v in drawn.items()}


def reference(x, w_gate, w_up, w_down):
    gate = jnp.dot(x, w_gate, preferred_element_type=jnp.float32)
    up = jnp.dot(x, w_up, preferred_element_type=jnp.float32)
    hidden = (jax.nn.silu(gate) * up).astype(jnp.bfloat16)
    return jnp.dot(hidden, w_down, preferred_element_type=jnp.float32).astype(jnp.bfloat16)
```

```python
import functools
import math

import jax
import jax.numpy as jnp
from jax import lax
from jax.experimental import pallas as pl
from jax.experimental.pallas import tpu as pltpu
from jax.sharding import PartitionSpec as P

MESH = pl.DeviceIdType.MESH
RINGS = 4
HALVES = 2
TILE_F = 256
TILE_D = 512


def neighbours(n):
    side = math.isqrt(n)
    me = lax.axis_index("tp")
    x, y = me // side, lax.rem(me, side)
    k = lax.rem(x + y, side)

    def first(p):
        row = p // side
        return lax.rem(lax.rem(p, side) - row + side, side) * side + row

    def second(p):
        col = p // side
        return col * side + lax.rem(lax.rem(p, side) - col + side, side)

    p1, p2 = y * side + k, x * side + k
    return (
        first(lax.rem(p1 + 1, n)),
        first(lax.rem(p1 + n - 1, n)),
        second(lax.rem(p2 + 1, n)),
        second(lax.rem(p2 + n - 1, n)),
    )


def kernel(n, x_ref, wg_ref, wu_ref, wd_ref, out_ref, xbuf, wg, wu, wd, xv, hidden, yin, yout,
           w_sem, l_sem, o_sem, xs_sem, xr_sem, ys_sem, yr_sem):
    rows, d = x_ref.shape
    ff = wg.shape[1]
    part = rows // RINGS
    half = d // HALVES
    nxt = neighbours(n)

    loads = [pltpu.make_async_copy(a, b, w_sem.at[i])
             for i, (a, b) in enumerate(((wg_ref, wg), (wu_ref, wu), (wd_ref, wd)))]
    for c in loads:
        c.start()
    yin[1] = jnp.zeros(yin.shape[1:], yin.dtype)

    barrier = pltpu.get_barrier_semaphore()
    for r in range(RINGS):
        pl.semaphore_signal(barrier, inc=1, device_id={"tp": nxt[r]}, device_id_type=MESH)
    pl.semaphore_wait(barrier, RINGS)

    def x_copy(s, r, src):
        return pltpu.make_async_remote_copy(
            src_ref=src, dst_ref=xbuf.at[s, r], send_sem=xs_sem.at[s, r], recv_sem=xr_sem.at[s, r],
            device_id={"tp": nxt[r]}, device_id_type=MESH)

    def y_copy(src_slot, dst_slot, h, r):
        band = pl.ds(r * part, part)
        return pltpu.make_async_remote_copy(
            src_ref=yout.at[src_slot, h, band], dst_ref=yin.at[dst_slot, h, band],
            send_sem=ys_sem.at[src_slot, h, r], recv_sem=yr_sem.at[dst_slot, h, r],
            device_id={"tp": nxt[r]}, device_id_type=MESH)

    for r in range(RINGS):
        x_copy(0, r, x_ref.at[pl.ds(r * part, part)]).start()
    for c in loads:
        c.wait()

    def step(s, carry):
        slot, other = lax.rem(s, 2), lax.rem(s + 1, 2)

        @pl.when(s < n)
        def _():
            for r in range(RINGS):
                x_copy(s - 1, r, xbuf.at[s - 1, r]).wait_recv()

                @pl.when(s < n - 1)
                def _():
                    x_copy(s, r, xbuf.at[s - 1, r]).start()

                pltpu.make_async_copy(xbuf.at[s - 1, r], xv.at[pl.ds(r * part, part)], l_sem.at[r]).start()

        @pl.when(s == n)
        def _():
            for r in range(RINGS):
                band = pl.ds(r * part, part)
                pltpu.make_async_copy(x_ref.at[band], xv.at[band], l_sem.at[r]).start()

        for r in range(RINGS):
            band = pl.ds(r * part, part)
            pltpu.make_async_copy(x_ref.at[band], xv.at[band], l_sem.at[r]).wait()

        @pl.loop(0, ff // TILE_F)
        def _(j):
            cols = pl.ds(pl.multiple_of(j * TILE_F, TILE_F), TILE_F)
            gate = jnp.dot(xv[...], wg[:, cols], preferred_element_type=jnp.float32)
            up = jnp.dot(xv[...], wu[:, cols], preferred_element_type=jnp.float32)
            hidden[:, cols] = (jax.nn.silu(gate) * up).astype(hidden.dtype)

        for h in range(HALVES):
            @pl.when(s >= 3)
            def _():
                for r in range(RINGS):
                    y_copy(slot, other, h, r).wait_send()

            @pl.when(s >= 2)
            def _():
                for r in range(RINGS):
                    y_copy(other, slot, h, r).wait_recv()

            @pl.loop(0, half // TILE_D)
            def _(j):
                cols = pl.ds(pl.multiple_of(j * TILE_D, TILE_D), TILE_D)
                wcols = pl.ds(pl.multiple_of(h * half + j * TILE_D, TILE_D), TILE_D)
                term = jnp.dot(hidden[...], wd[:, wcols], preferred_element_type=jnp.float32)
                total = term + yin[slot, h, :, cols].astype(jnp.float32)
                yout[slot, h, :, cols] = total.astype(yout.dtype)

            @pl.when(s < n)
            def _():
                for r in range(RINGS):
                    y_copy(slot, other, h, r).start()

            @pl.when(s == n)
            def _():
                pltpu.make_async_copy(yout.at[slot, h], out_ref.at[:, pl.ds(h * half, half)], o_sem.at[h]).start()

        return carry

    lax.fori_loop(1, n + 1, step, 0)

    for h in range(HALVES):
        pltpu.make_async_copy(yout.at[n % 2, h], out_ref.at[:, pl.ds(h * half, half)], o_sem.at[h]).wait()
        for r in range(RINGS):
            y_copy((n - 1) % 2, n % 2, h, r).wait_send()

    def drain(s, carry):
        for r in range(RINGS):
            x_copy(s, r, xbuf.at[s, r]).wait_send()
        return carry

    lax.fori_loop(0, n - 1, drain, 0)


def solution(mesh):
    n = mesh.shape["tp"]

    def step(x, w_gate, w_up, w_down):
        rows, d = x.shape
        ff = w_gate.shape[1]
        part, half = rows // RINGS, d // HALVES
        dt = x.dtype
        y, _ = pl.pallas_call(
            functools.partial(kernel, n),
            out_shape=(jax.ShapeDtypeStruct((rows, d), dt),
                       jax.ShapeDtypeStruct((n - 1, RINGS, part, d), dt)),
            in_specs=[pl.BlockSpec(memory_space=pltpu.HBM)] * 4,
            out_specs=[pl.BlockSpec(memory_space=pltpu.HBM)] * 2,
            scratch_shapes=[
                pltpu.VMEM((d, ff), dt),
                pltpu.VMEM((d, ff), dt),
                pltpu.VMEM((ff, d), dt),
                pltpu.VMEM((rows, d), dt),
                pltpu.VMEM((rows, ff), dt),
                pltpu.VMEM((2, HALVES, rows, half), dt),
                pltpu.VMEM((2, HALVES, rows, half), dt),
                pltpu.SemaphoreType.DMA((3,)),
                pltpu.SemaphoreType.DMA((RINGS,)),
                pltpu.SemaphoreType.DMA((HALVES,)),
                pltpu.SemaphoreType.DMA((n - 1, RINGS)),
                pltpu.SemaphoreType.DMA((n - 1, RINGS)),
                pltpu.SemaphoreType.DMA((2, HALVES, RINGS)),
                pltpu.SemaphoreType.DMA((2, HALVES, RINGS)),
            ],
            compiler_params=pltpu.CompilerParams(
                collective_id=0, has_side_effects=True, vmem_limit_bytes=60 * 2**20),
        )(x, w_gate, w_up, w_down)
        return y

    return jax.shard_map(
        step,
        mesh=mesh,
        in_specs=(P(("dp", "tp"), None), P(None, "tp"), P(None, "tp"), P("tp", None)),
        out_specs=P(("dp", "tp"), None),
        check_vma=False,
    )
```

```python
import functools
import math

import jax
import jax.numpy as jnp
from jax import lax
from jax.experimental import pallas as pl
from jax.experimental.pallas import tpu as pltpu
from jax.sharding import PartitionSpec as P

MESH = pl.DeviceIdType.MESH
ZROWS = 48
PIECES = 4
TILE_F = 512
TILE_D = 256


def kernel(n, x_ref, wg_ref, wu_ref, wd_ref, out_ref, xg, wdx,
           wg, wu, wgx, wux, xv, hid, hs, yin, yout, wt, rel,
           own_sem, stage_sem, wt_sem, out_sem, xs, xr, ws, wr, ds, dr, ys, yr, rs, rr):
    side = math.isqrt(n)
    ring = n // 2
    rows, d = x_ref.shape
    ff = wg.shape[1]
    half, quarter, width = rows // 2, ff // 4, d // PIECES
    srows = half - 2 * ZROWS
    tiles = width // TILE_D

    me, dp = lax.axis_index("tp"), lax.axis_index("dp")
    x, y = me // side, lax.rem(me, side)
    u = lax.rem(x - y + side, side)
    k, v = u // 2, lax.rem(u, 2)
    q = 2 * y + v
    m = lax.rem(q, 4)
    core = lax.rem(dp, 2)
    partner = dp + 1 - 2 * core

    def wrap(p):
        return lax.rem(p + 2 * ring, ring)

    def device(p):
        row = p // 2
        return lax.rem(row + 2 * k + lax.rem(p, 2), side) * side + row

    sp, sm = device(wrap(q + 1)), device(wrap(q - 1))
    cross = (lax.rem(x + 2 * v - 1 + side, side) * side + y, x * side + lax.rem(y + 1 - 2 * v + side, side))
    cp = cross[1] + v * (cross[0] - cross[1])
    cm = cross[0] + v * (cross[1] - cross[0])

    def remote(src, dst, send, recv, tp=None):
        device_id = {"dp": partner} if tp is None else {"tp": tp}
        return pltpu.make_async_remote_copy(
            src_ref=src, dst_ref=dst, send_sem=send, recv_sem=recv, device_id=device_id, device_id_type=MESH)

    def chunk(way, j):
        t = j // 2 + 1
        return (wrap(q - t), j % 2) if way == 0 else (wrap(q + t), 1 - j % 2)

    def hband(h):
        return pl.ds(h * half, half)

    def x_send(way, j):
        t = j // 2 + 1
        owner, h = (wrap(q - t + 1), j % 2) if way == 0 else (wrap(q + t - 1), 1 - j % 2)
        src = x_ref.at[hband(h)] if t == 1 else xg.at[owner, hband(h)]
        return remote(src, xg.at[owner, hband(h)], xs.at[j, way], xr.at[j, way], (sp, sm)[way])

    last = ring - 2

    def w_views(piece, index):
        if piece == 2:
            band = pl.ds(pl.multiple_of(index * quarter, quarter), quarter)
            return wd_ref.at[band], wdx.at[band]
        cols = pl.ds(pl.multiple_of(index * quarter, quarter), quarter)
        return (wg_ref, wu_ref)[piece].at[:, cols], (wgx, wux)[piece].at[:, cols]

    def w_send(piece, link):
        src, dst = w_views(piece, 2 * link + core)
        return remote(src, dst, ws.at[piece, link], wr.at[piece, link], cross[link])

    def w_share(piece, link):
        _, dst = w_views(piece, 2 * link + core)
        return remote(dst, dst, ds.at[piece, link], dr.at[piece, link])

    def pass_on(piece):
        for link in range(2):
            w_send(piece, link).wait_recv()
            w_share(piece, link).start()

    loads = [pltpu.make_async_copy(a, b, own_sem.at[i]) for i, (a, b) in enumerate(((wg_ref, wg), (wu_ref, wu)))]
    for c in loads:
        c.start()
    yin[1] = jnp.zeros(yin.shape[1:], yin.dtype)
    barrier = pltpu.get_barrier_semaphore()
    for tp in (sp, sm, cp, cm):
        pl.semaphore_signal(barrier, inc=1, device_id={"tp": tp}, device_id_type=MESH)
    pl.semaphore_signal(barrier, inc=1, device_id={"dp": partner}, device_id_type=MESH)
    pl.semaphore_wait(barrier, 5)
    for j in range(2):
        for way in range(2):
            x_send(way, j).start()
    for piece in range(3):
        for link in range(2):
            w_send(piece, link).start()

    def blocks(unit):
        if unit == 0:
            return (q, 0), (q, 1)
        return chunk(0, unit - 1), chunk(1, unit - 1)

    def stage(unit, slot):
        out = []
        for i, (owner, h) in enumerate(blocks(unit)):
            src = x_ref.at[hband(h)] if unit == 0 else xg.at[owner, hband(h)]
            out.append(pltpu.make_async_copy(src, xv.at[slot, hband(i)], stage_sem.at[slot, i]))
        return out

    def start(copies):
        for c in copies:
            c.start()

    def wait(copies):
        for c in copies:
            c.wait()

    def work(unit, slot, other):
        gates, ups = (wgx, wux) if other else (wg, wu)
        (o0, h0), (o1, h1) = blocks(unit)
        base = ff if other else 0

        @pl.loop(0, ff // TILE_F)
        def _(j):
            cols = pl.ds(pl.multiple_of(j * TILE_F, TILE_F), TILE_F)
            to = pl.ds(pl.multiple_of(base + j * TILE_F, TILE_F), TILE_F)
            gate = jnp.dot(xv[slot], gates[:, cols], preferred_element_type=jnp.float32)
            up = jnp.dot(xv[slot], ups[:, cols], preferred_element_type=jnp.float32)
            act = (jax.nn.silu(gate) * up).astype(hid.dtype)
            hid[o0, hband(h0), to] = act[:half]
            hid[o1, hband(h1), to] = act[half:]

    def arrive(j):
        for way in range(2):
            x_send(way, j).wait_recv()
            if j + 2 <= last:
                x_send(way, j + 2).start()

    def run(jobs):
        start(stage(jobs[0][0], 0))
        for i, (unit, other) in enumerate(jobs):
            wait(stage(unit, i % 2))
            if i + 1 < len(jobs):
                start(stage(jobs[i + 1][0], (i + 1) % 2))
            work(unit, i % 2, other)

    start(stage(0, 0))
    wait(loads)
    wait(stage(0, 0))
    work(0, 0, False)
    for j in range(2):
        arrive(j)
        run([(j + 1, False)])
    arrive(2)
    run([(3, False)])
    pass_on(0)
    arrive(3)
    start(stage(4, 0))
    wait(stage(4, 0))
    work(4, 0, False)
    pass_on(1)
    for piece in range(2):
        for link in range(2):
            w_share(piece, link).wait_recv()
    run([(0, True), (1, True)])
    arrive(4)
    run([(5, False), (2, True), (3, True)])
    arrive(5)
    run([(6, False)])
    pass_on(2)
    run([(4, True)])
    for link in range(2):
        w_share(2, link).wait_recv()

    offs = (0, srows, srows + ZROWS, half, half + srows, half + srows + ZROWS)
    sizes = (srows, ZROWS, ZROWS) * 2

    def fold(p):
        f = lax.rem(p, 4)
        return p + (f // 2) * (5 - 2 * f)

    def owner(r, s):
        if r == 0:
            return wrap(q - s)
        if r == 3:
            return wrap(q + s)
        shift = (0, 0, 2, 0, 1, 3)[r]
        p = fold(wrap(q - shift))
        return wrap(fold(wrap(p - s if r < 3 else p + s)) + shift)

    in12, in23 = lax.rem((m + 1) // 2, 2), m // 2

    def zband(way, index):
        return pl.ds(pl.multiple_of(way * half + srows + index * ZROWS, 8), ZROWS)

    def y_sends(slot, c):
        to = 1 - slot
        out = [remote(yout.at[slot, c, pl.ds(offs[r], sizes[r])], yin.at[to, c, pl.ds(offs[r], sizes[r])],
                      ys.at[slot, c, way], yr.at[to, c, r], (sp, sm)[way]) for way, r in ((0, 0), (1, 3))]
        for way, index, tp in ((0, in12, sp + v * (sm - sp)), (1, 1 - in23, sm + v * (sp - sm))):
            band = zband(way, index)
            out.append(remote(yout.at[slot, c, band], yin.at[to, c, band], ys.at[slot, c, 2 + way],
                              yr.at[to, c, 3 * way + 1 + index], tp))
        for way, index, tp in ((0, 1 - in12, cp), (1, in23, cm)):
            out.append(remote(yout.at[slot, c, zband(way, index)], rel.at[way, slot, c], ys.at[slot, c, 4 + way],
                              rr.at[way, slot, c], tp))
        return out

    def relays(slot, c):
        to = 1 - slot
        return [remote(rel.at[way, slot, c], yin.at[to, c, zband(way, index)], rs.at[way, slot, c],
                       yr.at[to, c, 3 * way + 1 + index], tp)
                for way, index, tp in ((0, in23, cp), (1, 1 - in12, cm))]

    def relay(slot, c):
        for way, copy in enumerate(relays(slot, c)):
            landed = rel.at[way, slot, c]
            remote(landed, landed, rs.at[way, slot, c], rr.at[way, slot, c], cp).wait_recv()
            copy.start()

    def y_waits(slot, c):
        for r in range(6):
            band = pl.ds(offs[r], sizes[r])
            remote(yin.at[slot, c, band], yin.at[slot, c, band], ys.at[slot, c, 0], yr.at[slot, c, r], sp).wait_recv()

    def w_tile(index, slot):
        cols = pl.ds(pl.multiple_of(index * TILE_D, TILE_D), TILE_D)
        return [pltpu.make_async_copy(ref.at[:, cols], wt.at[slot, pl.ds(i * ff, ff)], wt_sem.at[slot, i])
                for i, ref in enumerate((wd_ref, wdx))]

    ahead = tiles - 1
    for i in range(ahead):
        start(w_tile(i, i))

    def out_copy(slot, c):
        return pltpu.make_async_copy(yout.at[slot, c], out_ref.at[:, pl.ds(c * width, width)], out_sem.at[c])

    def step(s, carry):
        slot = lax.rem(s, 2)
        for r in range(6):
            band = pl.ds(offs[r], sizes[r])
            hs[band] = hid[owner(r, s), band]

        for c in range(PIECES):
            @pl.when(s >= 3)
            def _():
                for copy in y_sends(slot, c):
                    copy.wait_send()

            @pl.when(s >= 2)
            def _():
                y_waits(slot, c)

            @pl.loop(0, tiles)
            def _(i):
                wait(w_tile(0, i))

                @pl.when((s < ring) | (c * tiles + i + ahead < PIECES * tiles))
                def _():
                    start(w_tile(lax.rem(c * tiles + i + ahead, PIECES * tiles), lax.rem(i + ahead, tiles)))

                cols = pl.ds(pl.multiple_of(i * TILE_D, TILE_D), TILE_D)
                term = jnp.dot(hs[...], wt[i], preferred_element_type=jnp.float32)
                total = term + yin[slot, c, :, cols].astype(jnp.float32)
                yout[slot, c, :, cols] = total.astype(yout.dtype)

            @pl.when(s >= 2)
            def _():
                for copy in relays(1 - slot, c):
                    copy.wait_send()

            @pl.when(s < ring)
            def _():
                start(y_sends(slot, c))
                if c:
                    relay(slot, c - 1)

            @pl.when(s == ring)
            def _():
                out_copy(slot, c).start()

        @pl.when(s == 1)
        def _():
            run([(5, True)])

        @pl.when(s == 2)
        def _():
            arrive(last)
            run([(last + 1, False)])

        @pl.when(s < ring)
        def _():
            relay(slot, PIECES - 1)

        @pl.when(s == 1)
        def _():
            run([(6, True)])

        @pl.when(s == 2)
        def _():
            run([(last + 1, True)])

        return carry

    lax.fori_loop(1, ring + 1, step, 0)

    for c in range(PIECES):
        for copy in y_sends((ring - 1) % 2, c):
            copy.wait_send()
        out_copy(ring % 2, c).wait()
    for way in range(2):
        for j in range(last + 1):
            x_send(way, j).wait_send()
    for piece in range(3):
        for link in range(2):
            w_send(piece, link).wait_send()
            w_share(piece, link).wait_send()


def solution(mesh):
    n = mesh.shape["tp"]
    ring = n // 2

    def step(x, w_gate, w_up, w_down):
        rows, d = x.shape
        ff = w_gate.shape[1]
        dt = x.dtype
        width = d // PIECES
        dma = pltpu.SemaphoreType.DMA
        y, _, _ = pl.pallas_call(
            functools.partial(kernel, n),
            out_shape=(jax.ShapeDtypeStruct((rows, d), dt),
                       jax.ShapeDtypeStruct((ring, rows, d), dt),
                       jax.ShapeDtypeStruct((ff, d), dt)),
            in_specs=[pl.BlockSpec(memory_space=pltpu.HBM)] * 4,
            out_specs=[pl.BlockSpec(memory_space=pltpu.HBM)] * 3,
            scratch_shapes=[
                pltpu.VMEM((d, ff), dt),
                pltpu.VMEM((d, ff), dt),
                pltpu.VMEM((d, ff), dt),
                pltpu.VMEM((d, ff), dt),
                pltpu.VMEM((2, rows, d), dt),
                pltpu.VMEM((ring, rows, 2 * ff), dt),
                pltpu.VMEM((rows, 2 * ff), dt),
                pltpu.VMEM((2, PIECES, rows, width), dt),
                pltpu.VMEM((2, PIECES, rows, width), dt),
                pltpu.VMEM((width // TILE_D, 2 * ff, TILE_D), dt),
                pltpu.VMEM((2, 2, PIECES, ZROWS, width), dt),
                dma((2,)),
                dma((2, 2)),
                dma((width // TILE_D, 2)),
                dma((PIECES,)),
                dma((ring - 1, 2)),
                dma((ring - 1, 2)),
                dma((3, 2)),
                dma((3, 2)),
                dma((3, 2)),
                dma((3, 2)),
                dma((2, PIECES, 6)),
                dma((2, PIECES, 6)),
                dma((2, 2, PIECES)),
                dma((2, 2, PIECES)),
            ],
            compiler_params=pltpu.CompilerParams(
                collective_id=0, has_side_effects=True, vmem_limit_bytes=67_000_000),
        )(x, w_gate, w_up, w_down)
        return y

    return jax.shard_map(
        step,
        mesh=mesh,
        in_specs=(P(("dp", "tp"), None), P(None, "tp"), P(None, "tp"), P("tp", None)),
        out_specs=P(("dp", "tp"), None),
        check_vma=False,
    )
```
